32 devices in a mesh: dp: 8 (over z, y), tensor: 4 (over x, core).
Axes of the slice: x: 2, y: 2, z: 4, core: 2. Of those that a mesh axis runs over, the one named last changes fastest.
Arguments:
- tokens_in: bfloat16 [1024, 4096], P(('dp', 'tensor')), may hold values from -6 to 6
- grad_out: bfloat16 [1024, 4096], P(('dp', 'tensor')), may hold values from -6 to 6
- gate_pre: bfloat16 [1024, 7168], P('dp', 'tensor'), may hold values from -6 to 6
- up_pre: bfloat16 [1024, 7168], P('dp', 'tensor'), may hold values from -6 to 6
- gate_weight: bfloat16 [4096, 7168], P('dp', 'tensor'), may hold values from -0.09375 to 0.09375
- up_weight: bfloat16 [4096, 7168], P('dp', 'tensor'), may hold values from -0.09375 to 0.09375
- down_weight: bfloat16 [7168, 4096], P('tensor', 'dp'), may hold values from -0.0625 to 0.0625
- norm_gain: float32 [4096], replicated, may hold values from 0.1 to 1.9
Outputs:
- input_grad: bfloat16 [1024, 4096], P(('dp', 'tensor'))
- gain_grad: float32 [4096], replicated
- down_grad: bfloat16 [7168, 4096], P('tensor', 'dp')
The draws below stay inside these ranges and needn't reach their ends.
All inputs are finite; a program needn't handle non-finite values.
Results may differ from the reference program's by a relative error of at most 0.015.
Values may be sent and summed in bfloat16 or wider, within the bound.
No kernel may reach another device: no remote copies, remote signals or barrier semaphores. Data moves between devices by JAX's collectives and lax.ppermute only.
A program may use at most 64 MiB of HBM per device.

```python
import jax
import jax.numpy as jnp
from jax import lax

D = 4096
FF = 7168
TOKENS = 1024
N_TENSOR = 4


def block_levels(key, extent, shards, smallest, top_value):
    factor_of, own = 1.0, jax.random.fold_in(key, 6)
    for dim, parts in shards:
        heights = jnp.exp(jax.random.uniform(jax.random.fold_in(own, dim), (parts,), jnp.float32, smallest / len(shards), top_value / len(shards)))
        factor_of = factor_of * jnp.repeat(heights, extent[dim] // parts).reshape([-1 if axis == dim else 1 for axis in range(len(extent))])
    return factor_of


def gaussian(rng, dims, deviation, most, pieces=(), kind=jnp.bfloat16):
    array = jax.random.normal(rng, dims, jnp.float32) * deviation
    if len(pieces) > 0:
        array = block_levels(rng, dims, pieces, -0.22, 0.18) * array
    return jnp.clip(array, min=-most, max=most).astype(kind)


def setup_inputs(seed: int = 0) -> dict:
    keys = jax.random.split(jax.random.key(seed), 9)
    return {
        "tokens_in": gaussian(keys[0], (TOKENS, D), 1.0, 6.0, ((0, 32),)),
        "grad_out": gaussian(keys[1], (TOKENS, D), 1.0, 6.0, ((0, 32),)),
        "gate_pre": gaussian(keys[2], (TOKENS, FF), 1.0, 6.0, ((0, 8), (1, 4))),
        "up_pre": gaussian(keys[3], (TOKENS, FF), 1.0, 6.0, ((0, 8), (1, 4))),
        "gate_weight": gaussian(keys[4], (D, FF), D ** -0.5, 0.09375, ((0, 8), (1, 4))),
        "up_weight": gaussian(keys[5], (D, FF), D ** -0.5, 0.09375, ((0, 8), (1, 4))),
        "down_weight": gaussian(keys[6], (FF, D), FF ** -0.5, 0.0625, ((0, 4), (1, 8))),
        "norm_gain": jnp.clip(1.0 + 0.18 * jax.random.normal(keys[7], (D,), jnp.float32), 0.1, 1.9),
    }


def reference(tokens_in, grad_out, gate_pre, up_pre, gate_weight, up_weight, down_weight, norm_gain):
    gate_value = gate_pre.astype(jnp.float32)
    up_value = up_pre.astype(jnp.float32)
    gate_sigmoid = jax.nn.sigmoid(gate_value)
    gate_silu = gate_value * gate_sigmoid
    act = (gate_silu * up_value).astype(jnp.bfloat16)
    grad_act = jnp.dot(grad_out, down_weight.T, preferred_element_type=jnp.float32)
    grad_gate = (grad_act * up_value * gate_sigmoid * (1.0 + gate_value * (1.0 - gate_sigmoid))).astype(jnp.bfloat16)
    grad_up = (grad_act * gate_silu).astype(jnp.bfloat16)
    down_grad = jnp.dot(act.T, grad_out, preferred_element_type=jnp.float32).astype(jnp.bfloat16)
    width = FF // N_TENSOR

    def add_shard(total, index):
        start = index * width
        gate_cols = lax.dynamic_slice_in_dim(grad_gate, start, width, 1)
        up_cols = lax.dynamic_slice_in_dim(grad_up, start, width, 1)
        gate_part = lax.dynamic_slice_in_dim(gate_weight, start, width, 1)
        up_part = lax.dynamic_slice_in_dim(up_weight, start, width, 1)
        part = jnp.dot(gate_cols, gate_part.T, preferred_element_type=jnp.float32)
        part = part + jnp.dot(up_cols, up_part.T, preferred_element_type=jnp.float32)
        return (total + lax.optimization_barrier(part.astype(jnp.bfloat16)).astype(jnp.float32), None)
    grad_norm, unused_two = lax.scan(add_shard, jnp.zeros((TOKENS, D), jnp.float32), jnp.arange(N_TENSOR, dtype=jnp.int32))
    inputs = tokens_in.astype(jnp.float32)
    inv_rms = lax.rsqrt(lax.optimization_barrier(jnp.mean(inputs * inputs, axis=1, keepdims=True)) + 1e-05)
    normed = inputs * inv_rms
    gain_grad = lax.optimization_barrier(jnp.sum(grad_norm * normed, axis=0))
    scaled = grad_norm * norm_gain
    inner = lax.optimization_barrier(jnp.mean(scaled * normed, axis=1, keepdims=True))
    input_grad = (grad_out.astype(jnp.float32) + inv_rms * (scaled - normed * inner)).astype(jnp.bfloat16)
    return (input_grad, gain_grad, down_grad)
```

```python
import jax
import jax.numpy as jnp
from jax import lax
from jax.sharding import PartitionSpec as P


BF16, F32 = jnp.bfloat16, jnp.float32


def make_per_device(mesh):
    groups, width = mesh.shape["dp"], mesh.shape["tensor"]
    na, nr = groups // 2, width // 2

    def ring(k):
        return [(a * 2 + b, (a + k) % na * 2 + b) for a in range(na) for b in range(2)]

    def move_a(value, k):
        return lax.ppermute(value, "dp", ring(k % na))

    def move_core(value):
        return lax.ppermute(value, "tensor", [(t, t ^ 1) for t in range(width)])

    def move_pair(value):
        return lax.ppermute(value, "dp", [(d, d ^ 1) for d in range(groups)])

    def move_br(value, kb, kr):
        pairs = []
        for d in range(groups):
            for r in range(nr):
                for c in range(2):
                    pairs.append(
                        (d * width + r * 2 + c, (d ^ kb) * width + (r + kr) % nr * 2 + c)
                    )
        return lax.ppermute(value, ("dp", "tensor"), pairs)

    def swap(value):
        half = value.shape[-1] // 2
        return jnp.concatenate((value[..., half:], value[..., :half]), axis=-1)

    def per_device(
        tokens_in, grad_out, gate_pre, up_pre, gate_weight, up_weight, down_weight, norm_gain
    ):
        rows, features = grad_out.shape
        hidden = gate_pre.shape[1] // 2
        own = down_weight.shape[1]
        pair = own * 2
        group = rows * width
        data, tensor = lax.axis_index("dp"), lax.axis_index("tensor")
        a, b = data // 2, data % 2
        r, c = tensor // 2, tensor % 2
        first = b == 0

        def by_distance(value):
            twice = jnp.concatenate((value, value), axis=1)
            rolled = lax.dynamic_slice_in_dim(twice, a * pair, features, 1)
            rolled = rolled.reshape(rows, na, 2, own)
            return jnp.where(first, rolled, rolled[:, :, ::-1]).reshape(rows, na, pair)

        out_blocks = by_distance(grad_out)
        near = jnp.stack([move_a(out_blocks[:, k], k) if k else out_blocks[:, 0] for k in range(na)])
        near_swapped = swap(near)
        grid = [
            [
                near if kb == 0 and kr == 0 else move_br(near_swapped if kb else near, kb, kr)
                for kr in range(nr)
            ]
            for kb in range(2)
        ]
        mine = jnp.stack([jnp.stack(line) for line in grid])
        both = jnp.stack((mine, move_core(mine)))
        every_out = both.transpose(3, 1, 2, 0, 4, 5).reshape(na * 2 * group, pair)

        def halves(value):
            low, high = value[..., :hidden], value[..., hidden:]
            return jnp.where(first, low, high), jnp.where(first, high, low)

        def relative_rows(value):
            blocks = value.reshape(width, rows, value.shape[1])
            return jnp.concatenate(
                [
                    lax.dynamic_index_in_dim(blocks, (r - kr + nr) % nr * 2 + (c ^ kc), 0, False)
                    for kr in range(nr)
                    for kc in range(2)
                ]
            )

        gate_keep, gate_give = halves(relative_rows(gate_pre))
        up_keep, up_give = halves(relative_rows(up_pre))
        pre_keep = jnp.stack((gate_keep, up_keep))
        pre_give = move_pair(jnp.stack((gate_give, up_give)))

        down_rows = down_weight.reshape(2, hidden, own)
        down_keep = lax.dynamic_index_in_dim(down_rows, b, 0, False)
        down_give = lax.dynamic_index_in_dim(down_rows, 1 - b, 0, False)
        down_pair = jnp.concatenate((down_keep, move_pair(down_give)), axis=1)

        gate_w_keep, gate_w_give = halves(gate_weight)
        up_w_keep, up_w_give = halves(up_weight)
        weight_keep = jnp.stack((gate_w_keep, up_w_keep))
        weight_give = move_pair(jnp.stack((gate_w_give, up_w_give)))
        weight_pair = jnp.concatenate((weight_keep, weight_give), axis=1)

        pre_keeps, pre_gives = [pre_keep], [pre_give]
        for _ in range(na - 1):
            pre_keeps.append(move_a(pre_keeps[-1], 1))
            pre_gives.append(move_a(pre_gives[-1], 1))

        partial = lax.dot_general(
            every_out, down_pair, (((1,), (1,)), ((), ())), preferred_element_type=F32
        ).astype(BF16).reshape(na, 2 * group, hidden)
        running = partial[1]
        for step in range(1, na):
            running = (
                move_a(running, 1).astype(F32) + partial[(step + 1) % na].astype(F32)
            ).astype(BF16)

        acts, grads = [], [running]
        for _ in range(na - 1):
            grads.append(move_a(grads[-1], 1))
        norm_blocks = []
        inputs = tokens_in.astype(F32)
        inv_rms = lax.rsqrt(jnp.mean(inputs * inputs, axis=1, keepdims=True) + 1e-05)
        normed = inputs * inv_rms
        normed_blocks = by_distance(normed)
        gain_part = jnp.zeros((pair,), F32)
        for k in range(na):
            value = jnp.concatenate((pre_keeps[k], pre_gives[k]), axis=1).astype(F32)
            gate_value, up_value = value[0], value[1]
            gate_sigmoid = jax.nn.sigmoid(gate_value)
            gate_silu = gate_value * gate_sigmoid
            acts.append((gate_silu * up_value).astype(BF16))
            grad_act = grads[k].astype(F32)
            grad_gate = (
                grad_act * up_value * gate_sigmoid * (1.0 + gate_value * (1.0 - gate_sigmoid))
            ).astype(BF16)
            grad_up = (grad_act * gate_silu).astype(BF16)
            norm_part = jnp.einsum(
                "grf,gdf->rd",
                jnp.stack((grad_gate, grad_up)),
                weight_pair,
                preferred_element_type=F32,
            ).astype(BF16)
            norm_part = norm_part.reshape(2, nr, 2, rows, pair)
            cores = (
                norm_part[:, :, 0].astype(F32) + move_core(norm_part[:, :, 1]).astype(F32)
            ).astype(BF16)
            total = cores[0, 0].astype(F32)
            for kb in range(2):
                for kr in range(nr):
                    if kb or kr:
                        piece = cores[kb, kr]
                        total = total + move_br(swap(piece) if kb else piece, kb, -kr).astype(F32)
            their_normed = move_a(normed_blocks[:, k], k) if k else normed_blocks[:, 0]
            gain_part = gain_part + jnp.sum(total * their_normed, axis=0)
            total = total.astype(BF16)
            norm_blocks.append(move_a(total, -k) if k else total)

        down_both = lax.dot_general(
            jnp.concatenate(acts), every_out, (((0,), (0,)), ((), ())), preferred_element_type=F32
        ).astype(BF16)
        down_mine, down_theirs = down_both[:, :own], move_pair(down_both[:, own:])
        down_grad = jnp.where(
            first,
            jnp.concatenate((down_mine, down_theirs)),
            jnp.concatenate((down_theirs, down_mine)),
        )

        gain = gain_part + move_core(gain_part)
        gain_sum = gain
        for kb in range(2):
            for kr in range(nr):
                if kb or kr:
                    gain_sum = gain_sum + move_br(swap(gain) if kb else gain, kb, kr)

        def natural(blocks, axis):
            value = jnp.stack(blocks, axis=axis)
            value = value.reshape(value.shape[:-1] + (2, own))
            value = jnp.where(first, value, jnp.flip(value, -2))
            value = value.reshape(value.shape[:axis] + (features,))
            twice = jnp.concatenate((value, value), axis=-1)
            return lax.dynamic_slice_in_dim(twice, (na - a) % na * pair, features, axis)

        gain_grad = natural([move_a(gain_sum, -k) if k else gain_sum for k in range(na)], 0)
        grad_norm = natural(norm_blocks, 1).astype(F32)
        scaled = grad_norm * norm_gain
        inner = jnp.mean(scaled * normed, axis=1, keepdims=True)
        input_grad = (grad_out.astype(F32) + inv_rms * (scaled - normed * inner)).astype(BF16)
        return (input_grad, gain_grad, down_grad)

    return per_device


def solution(mesh):
    return jax.shard_map(
        make_per_device(mesh),
        mesh=mesh,
        in_specs=(
            P(("dp", "tensor"), None),
            P(("dp", "tensor"), None),
            P("dp", "tensor"),
            P("dp", "tensor"),
            P("dp", "tensor"),
            P("dp", "tensor"),
            P("tensor", "dp"),
            P(),
        ),
        out_specs=(P(("dp", "tensor"), None), P(), P("tensor", "dp")),
        check_vma=False,
    )
```

```python
import jax
import jax.numpy as jnp
from jax import lax
from jax.sharding import PartitionSpec as P


BF16, F32 = jnp.bfloat16, jnp.float32


def make_per_device(mesh):
    groups, width = mesh.shape["dp"], mesh.shape["tensor"]
    na, nr = groups // 2, width // 2

    def ring(k):
        return [(a * 2 + b, (a + k) % na * 2 + b) for a in range(na) for b in range(2)]

    def move_a(value, k):
        return lax.ppermute(value, "dp", ring(k % na))

    def move_core(value):
        return lax.ppermute(value, "tensor", [(t, t ^ 1) for t in range(width)])

    def move_pair(value):
        return lax.ppermute(value, "dp", [(d, d ^ 1) for d in range(groups)])

    def move_br(value, kb, kr):
        pairs = []
        for d in range(groups):
            for r in range(nr):
                for c in range(2):
                    pairs.append(
                        (d * width + r * 2 + c, (d ^ kb) * width + (r + kr) % nr * 2 + c)
                    )
        return lax.ppermute(value, ("dp", "tensor"), pairs)

    def per_device(
        tokens_in, grad_out, gate_pre, up_pre, gate_weight, up_weight, down_weight, norm_gain
    ):
        rows, features = grad_out.shape
        hidden = gate_pre.shape[1] // 2
        own = down_weight.shape[1]
        pair = own * 2
        group = rows * width
        data, tensor = lax.axis_index("dp"), lax.axis_index("tensor")
        a, b = data // 2, data % 2
        r, c = tensor // 2, tensor % 2
        first = b == 0

        def block_of(value, k):
            return lax.dynamic_slice_in_dim(value, (a + k) % na * pair, pair, 1)

        def ordered(kept, given, axis):
            return jnp.where(
                first,
                jnp.concatenate((kept, given), axis=axis),
                jnp.concatenate((given, kept), axis=axis),
            )

        def halves(value):
            low, high = value[..., :hidden], value[..., hidden:]
            return jnp.where(first, low, high), jnp.where(first, high, low)

        def relative_rows(value):
            blocks = value.reshape(width, rows, value.shape[1])
            return jnp.concatenate(
                [
                    lax.dynamic_index_in_dim(blocks, (r - kr + nr) % nr * 2 + (c ^ kc), 0, False)
                    for kr in range(nr)
                    for kc in range(2)
                ]
            )

        gate_keep, gate_give = halves(relative_rows(gate_pre))
        up_keep, up_give = halves(relative_rows(up_pre))
        pre = [[jnp.stack((gate_keep, up_keep)), move_pair(jnp.stack((gate_give, up_give)))]]

        down_rows = down_weight.reshape(2, hidden, own)
        down_keep = lax.dynamic_index_in_dim(down_rows, b, 0, False)
        down_give = lax.dynamic_index_in_dim(down_rows, 1 - b, 0, False)
        down_pair = ordered(down_keep, move_pair(down_give), 1)

        inputs = tokens_in.astype(F32)
        inv_rms = lax.rsqrt(jnp.mean(inputs * inputs, axis=1, keepdims=True) + 1e-05)
        normed = inputs * inv_rms
        terms, rest = [], inv_rms
        for _ in range(3):
            terms.append(lax.reduce_precision(rest, 8, 7))
            rest = rest - terms[-1]
        extra = jnp.concatenate(terms + [jnp.zeros((rows, 125), F32)], axis=1).astype(BF16)

        near = jnp.stack(
            [move_a(block_of(grad_out, k), k) if k else block_of(grad_out, 0) for k in range(na)]
        )
        every_out = []
        for kb in range(2):
            mine = jnp.stack(
                [near if kb == 0 and kr == 0 else move_br(near, kb, kr) for kr in range(nr)]
            )
            both = jnp.stack((mine, move_core(mine)))
            every_out.append(both.transpose(2, 1, 0, 3, 4).reshape(na, group, pair))

        near_normed = []
        for k in range(na):
            message = jnp.concatenate((block_of(tokens_in, k), extra), axis=1)
            if k:
                message = move_a(message, k)
            near_normed.append(message)

        gate_w_keep, gate_w_give = halves(gate_weight)
        up_w_keep, up_w_give = halves(up_weight)
        weight_keep = jnp.stack((gate_w_keep, up_w_keep))
        weight_give = move_pair(jnp.stack((gate_w_give, up_w_give)))
        weight_pair = jnp.zeros((2, pair, hidden), BF16)
        weight_pair = lax.dynamic_update_slice_in_dim(weight_pair, weight_keep, b * own, 1)
        weight_pair = lax.dynamic_update_slice_in_dim(weight_pair, weight_give, (1 - b) * own, 1)

        for _ in range(1, na):
            pre.append([move_a(pre[-1][kb], 1) for kb in range(2)])

        grads = [[None, None] for _ in range(na)]
        for kb in range(2):
            partial = lax.dot_general(
                every_out[kb].reshape(na * group, pair),
                down_pair,
                (((1,), (1,)), ((), ())),
                preferred_element_type=F32,
            ).astype(BF16).reshape(na, group, hidden)
            running = partial[1]
            for step in range(1, na):
                running = (
                    move_a(running, 1).astype(F32)
                    + partial[(step + 1) % na].astype(F32)
                ).astype(BF16)
            grads[0][kb] = running
            for k in range(1, na):
                grads[k][kb] = move_a(grads[k - 1][kb], 1)

        acts, norm_blocks = [], []
        gain_part = jnp.zeros((pair,), F32)
        for k in range(na):
            value = jnp.concatenate(pre[k], axis=1).astype(F32)
            gate_value, up_value = value[0], value[1]
            gate_sigmoid = jax.nn.sigmoid(gate_value)
            gate_silu = gate_value * gate_sigmoid
            acts.append((gate_silu * up_value).astype(BF16))
            grad_act = jnp.concatenate(grads[k]).astype(F32)
            grad_gate = (
                grad_act * up_value * gate_sigmoid * (1.0 + gate_value * (1.0 - gate_sigmoid))
            ).astype(BF16)
            grad_up = (grad_act * gate_silu).astype(BF16)
            norm_part = jnp.einsum(
                "grf,gdf->rd",
                jnp.stack((grad_gate, grad_up)),
                weight_pair,
                preferred_element_type=F32,
            ).astype(BF16)
            norm_part = norm_part.reshape(2, nr, 2, rows, pair)
            across = move_core(norm_part[:, :, 1])
            cores = (norm_part[:, :, 0].astype(F32) + across.astype(F32)).astype(BF16)
            total = cores[0, 0].astype(F32)
            for kb in range(2):
                for kr in range(nr):
                    if kb or kr:
                        piece = cores[kb, kr]
                        piece = move_br(piece, kb, -kr)
                        total = total + piece.astype(F32)
            message, total = lax.optimization_barrier((near_normed[k], total))
            tail = message[:, pair:].astype(F32)
            their_inputs = message[:, :pair]
            their_inv = tail[:, 0:1] + tail[:, 1:2] + tail[:, 2:3]
            their_normed = their_inputs.astype(F32) * their_inv
            gain_part = gain_part + jnp.sum(total * their_normed, axis=0)
            total = total.astype(BF16)
            norm_blocks.append(move_a(total, -k) if k else total)

        down_both = lax.dot_general(
            jnp.concatenate(acts),
            jnp.concatenate(every_out, axis=1).reshape(na * 2 * group, pair),
            (((0,), (0,)), ((), ())),
            preferred_element_type=F32,
        ).astype(BF16)
        low, high = down_both[:, :own], down_both[:, own:]
        theirs = move_pair(jnp.where(first, high, low))
        down_grad = jnp.zeros((2 * hidden, own), BF16)
        mine = jnp.where(first, low, high)
        down_grad = lax.dynamic_update_slice_in_dim(down_grad, mine, b * hidden, 0)
        down_grad = lax.dynamic_update_slice_in_dim(down_grad, theirs, (1 - b) * hidden, 0)

        gain = gain_part + move_core(gain_part)
        gain_sum = gain
        for kb in range(2):
            for kr in range(nr):
                if kb or kr:
                    gain_sum = gain_sum + move_br(gain, kb, kr)

        def natural(blocks, axis):
            twice = jnp.concatenate(blocks + blocks, axis=axis)
            return lax.dynamic_slice_in_dim(twice, (na - a) % na * pair, features, axis)

        gain_grad = natural([move_a(gain_sum, -k) if k else gain_sum for k in range(na)], 0)
        grad_norm = natural(norm_blocks, 1).astype(F32)
        scaled = grad_norm * norm_gain
        inner = jnp.mean(scaled * normed, axis=1, keepdims=True)
        input_grad = (grad_out.astype(F32) + inv_rms * (scaled - normed * inner)).astype(BF16)
        return (input_grad, gain_grad, down_grad)

    return per_device


def solution(mesh):
    inner = make_per_device(mesh)

    return jax.shard_map(
        inner,
        mesh=mesh,
        in_specs=(
            P(("dp", "tensor"), None),
            P(("dp", "tensor"), None),
            P("dp", "tensor"),
            P("dp", "tensor"),
            P("dp", "tensor"),
            P("dp", "tensor"),
            P("tensor", "dp"),
            P(),
        ),
        out_specs=(P(("dp", "tensor"), None), P(), P("tensor", "dp")),
        check_vma=False,
    )
```

```python
import jax
import jax.numpy as jnp
from jax import lax
from jax.sharding import PartitionSpec as P


BF16, F32 = jnp.bfloat16, jnp.float32


def make_per_device(mesh):
    groups, width = mesh.shape["dp"], mesh.shape["tensor"]
    na, nr = groups // 2, width // 2

    def ring(k):
        return [(a * 2 + b, (a + k) % na * 2 + b) for a in range(na) for b in range(2)]

    def move_a(value, k):
        return lax.ppermute(value, "dp", ring(k % na))

    def move_core(value):
        return lax.ppermute(value, "tensor", [(t, t ^ 1) for t in range(width)])

    def move_pair(value):
        return lax.ppermute(value, "dp", [(d, d ^ 1) for d in range(groups)])

    def move_br(value, kb, kr):
        pairs = []
        for d in range(groups):
            for r in range(nr):
                for c in range(2):
                    pairs.append(
                        (d * width + r * 2 + c, (d ^ kb) * width + (r + kr) % nr * 2 + c)
                    )
        return lax.ppermute(value, ("dp", "tensor"), pairs)

    def per_device(
        tokens_in, grad_out, gate_pre, up_pre, gate_weight, up_weight, down_weight, norm_gain
    ):
        rows, features = grad_out.shape
        hidden = gate_pre.shape[1] // 2
        own = down_weight.shape[1]
        pair = own * 2
        group = rows * width
        data, tensor = lax.axis_index("dp"), lax.axis_index("tensor")
        a, b = data // 2, data % 2
        r, c = tensor // 2, tensor % 2
        first = b == 0

        def block_of(value, k):
            return lax.dynamic_slice_in_dim(value, (a + k) % na * pair, pair, 1)

        def ordered(kept, given, axis):
            return jnp.where(
                first,
                jnp.concatenate((kept, given), axis=axis),
                jnp.concatenate((given, kept), axis=axis),
            )

        down_rows = down_weight.reshape(2, hidden, own)
        down_keep = lax.dynamic_index_in_dim(down_rows, b, 0, False)
        down_give = lax.dynamic_index_in_dim(down_rows, 1 - b, 0, False)
        down_pair = ordered(down_keep, move_pair(down_give), 1)

        def halves(value):
            low, high = value[..., :hidden], value[..., hidden:]
            return jnp.where(first, low, high), jnp.where(first, high, low)

        def relative_rows(value):
            blocks = value.reshape(width, rows, value.shape[1])
            return jnp.concatenate(
                [
                    lax.dynamic_index_in_dim(blocks, (r - kr + nr) % nr * 2 + (c ^ kc), 0, False)
                    for kr in range(nr)
                    for kc in range(2)
                ]
            )

        gate_keep, gate_give = halves(relative_rows(gate_pre))
        up_keep, up_give = halves(relative_rows(up_pre))
        pre = [[jnp.stack((gate_keep, up_keep)), move_pair(jnp.stack((gate_give, up_give)))]]

        inputs = tokens_in.astype(F32)
        inv_rms = lax.rsqrt(jnp.mean(inputs * inputs, axis=1, keepdims=True) + 1e-05)
        normed = inputs * inv_rms
        terms, rest = [], inv_rms
        for _ in range(3):
            terms.append(lax.reduce_precision(rest, 8, 7))
            rest = rest - terms[-1]
        extra = jnp.concatenate(terms + [jnp.zeros((rows, 125), F32)], axis=1).astype(BF16)

        near = jnp.stack(
            [move_a(block_of(grad_out, k), k) if k else block_of(grad_out, 0) for k in range(na)]
        )
        every_out = []
        for kb in range(2):
            pieces = [near if kb == 0 and kr == 0 else move_br(near, kb, kr) for kr in range(nr)]
            mine = jnp.stack(pieces)
            both = jnp.stack((mine, move_core(mine)))
            every_out.append(both.transpose(2, 1, 0, 3, 4).reshape(na, group, pair))

        gate_w_keep, gate_w_give = halves(gate_weight)
        up_w_keep, up_w_give = halves(up_weight)
        weight_keep = jnp.stack((gate_w_keep, up_w_keep))
        weight_give = jnp.stack((gate_w_give, up_w_give))
        weight_give = move_pair(weight_give)
        weight_pair = jnp.zeros((2, pair, hidden), BF16)
        weight_pair = lax.dynamic_update_slice_in_dim(weight_pair, weight_keep, b * own, 1)
        weight_pair = lax.dynamic_update_slice_in_dim(weight_pair, weight_give, (1 - b) * own, 1)

        for _ in range(1, na):
            pre.append([move_a(pre[-1][kb], 1) for kb in range(2)])

        grads = [[None, None] for _ in range(na)]
        for kb in range(2):
            partial = lax.dot_general(
                every_out[kb].reshape(na * group, pair),
                down_pair,
                (((1,), (1,)), ((), ())),
                preferred_element_type=F32,
            ).astype(BF16).reshape(na, group, hidden)
            running = partial[1]
            for step in range(1, na):
                theirs = move_a(running, 1)
                running = (theirs.astype(F32) + partial[(step + 1) % na].astype(F32)).astype(BF16)
            grads[0][kb] = running
        late_inputs, late_extra, grads[0][1] = lax.optimization_barrier(
            (tokens_in, extra, grads[0][1])
        )
        near_normed = []
        for k in range(na):
            message = jnp.concatenate((block_of(late_inputs, k), late_extra), axis=1)
            if k:
                message = move_a(message, k)
            near_normed.append(message)
        for kb in range(2):
            for k in range(1, na):
                grads[k][kb] = move_a(grads[k - 1][kb], 1)

        pre_parts = [tuple(parts) for parts in pre]
        acts, norm_blocks = [], []
        gain_part = jnp.zeros((pair,), F32)
        for k in range(na):
            value = jnp.concatenate(pre_parts[k], axis=1).astype(F32)
            gate_value, up_value = value[0], value[1]
            gate_sigmoid = jax.nn.sigmoid(gate_value)
            gate_silu = gate_value * gate_sigmoid
            grad_act = jnp.concatenate(grads[k]).astype(F32)
            grad_gate = (
                grad_act * up_value * gate_sigmoid * (1.0 + gate_value * (1.0 - gate_sigmoid))
            ).astype(BF16)
            grad_up = (grad_act * gate_silu).astype(BF16)
            norm_part = jnp.einsum(
                "grf,gdf->rd",
                jnp.stack((grad_gate, grad_up)),
                weight_pair,
                preferred_element_type=F32,
            ).astype(BF16)
            norm_part = norm_part.reshape(2, nr, 2, rows, pair)
            across = move_core(norm_part[:, :, 1])
            cores = (norm_part[:, :, 0].astype(F32) + across.astype(F32)).astype(BF16)
            total = cores[0, 0].astype(F32)
            for kb in range(2):
                for kr in range(nr):
                    if kb or kr:
                        piece = cores[kb, kr]
                        piece = move_br(piece, kb, -kr)
                        total = total + piece.astype(F32)
            block = total.astype(BF16)
            norm_blocks.append(move_a(block, -k) if k else block)
            message, total = lax.optimization_barrier((near_normed[k], total))
            tail = message[:, pair:].astype(F32)
            their_inputs = message[:, :pair]
            their_inv = tail[:, 0:1] + tail[:, 1:2] + tail[:, 2:3]
            their_normed = their_inputs.astype(F32) * their_inv
            gain_part = gain_part + jnp.sum(total * their_normed, axis=0)

        for k in range(na):
            value = jnp.concatenate(pre_parts[k], axis=1).astype(F32)
            gate_value, up_value = value[0], value[1]
            acts.append((gate_value * jax.nn.sigmoid(gate_value) * up_value).astype(BF16))
        down_both = lax.dot_general(
            jnp.concatenate(acts),
            jnp.concatenate(every_out, axis=1).reshape(na * 2 * group, pair),
            (((0,), (0,)), ((), ())),
            preferred_element_type=F32,
        ).astype(BF16)
        low, high = down_both[:, :own], down_both[:, own:]
        theirs = move_pair(jnp.where(first, high, low))
        down_grad = jnp.zeros((2 * hidden, own), BF16)
        mine = jnp.where(first, low, high)
        down_grad = lax.dynamic_update_slice_in_dim(down_grad, mine, b * hidden, 0)
        down_grad = lax.dynamic_update_slice_in_dim(down_grad, theirs, (1 - b) * hidden, 0)

        gain = gain_part + move_core(gain_part)
        gain_sum = gain
        for kb in range(2):
            for kr in range(nr):
                if kb or kr:
                    gain_sum = gain_sum + move_br(gain, kb, kr)

        def natural(blocks, axis):
            twice = jnp.concatenate(blocks + blocks, axis=axis)
            return lax.dynamic_slice_in_dim(twice, (na - a) % na * pair, features, axis)

        gain_grad = natural([move_a(gain_sum, -k) if k else gain_sum for k in range(na)], 0)
        grad_norm = natural(norm_blocks, 1).astype(F32)
        scaled = grad_norm * norm_gain
        inner = jnp.mean(scaled * normed, axis=1, keepdims=True)
        step = inv_rms * (scaled - normed * inner)
        input_grad = (grad_out.astype(F32) + step).astype(BF16)
        return (input_grad, gain_grad, down_grad)

    return per_device


def solution(mesh):
    inner = make_per_device(mesh)

    return jax.shard_map(
        inner,
        mesh=mesh,
        in_specs=(
            P(("dp", "tensor"), None),
            P(("dp", "tensor"), None),
            P("dp", "tensor"),
            P("dp", "tensor"),
            P("dp", "tensor"),
            P("dp", "tensor"),
            P("tensor", "dp"),
            P(),
        ),
        out_specs=(P(("dp", "tensor"), None), P(), P("tensor", "dp")),
        check_vma=False,
    )
```

```python
import jax
import jax.numpy as jnp
from jax import lax
from jax.sharding import PartitionSpec as P


BF16, F32 = jnp.bfloat16, jnp.float32


def make_per_device(mesh):
    groups, width = mesh.shape["dp"], mesh.shape["tensor"]
    na, nr = groups // 2, width // 2

    def ring(k):
        return [(a * 2 + b, (a + k) % na * 2 + b) for a in range(na) for b in range(2)]

    def move_a(value, k):
        return lax.ppermute(value, "dp", ring(k % na))

    def move_core(value):
        return lax.ppermute(value, "tensor", [(t, t ^ 1) for t in range(width)])

    def move_pair(value):
        return lax.ppermute(value, "dp", [(d, d ^ 1) for d in range(groups)])

    def move_br(value, kb, kr):
        pairs = []
        for d in range(groups):
            for r in range(nr):
                for c in range(2):
                    pairs.append(
                        (d * width + r * 2 + c, (d ^ kb) * width + (r + kr) % nr * 2 + c)
                    )
        return lax.ppermute(value, ("dp", "tensor"), pairs)

    def per_device(
        tokens_in, grad_out, gate_pre, up_pre, gate_weight, up_weight, down_weight, norm_gain
    ):
        rows, features = grad_out.shape
        hidden = gate_pre.shape[1] // 2
        own = down_weight.shape[1]
        pair = own * 2
        group = rows * width
        data, tensor = lax.axis_index("dp"), lax.axis_index("tensor")
        a, b = data // 2, data % 2
        r, c = tensor // 2, tensor % 2
        first = b == 0

        def block_of(value, k):
            return lax.dynamic_slice_in_dim(value, (a + k) % na * pair, pair, 1)

        def ordered(kept, given, axis):
            return jnp.where(
                first,
                jnp.concatenate((kept, given), axis=axis),
                jnp.concatenate((given, kept), axis=axis),
            )

        down_rows = down_weight.reshape(2, hidden, own)
        down_keep = lax.dynamic_index_in_dim(down_rows, b, 0, False)
        down_give = lax.dynamic_index_in_dim(down_rows, 1 - b, 0, False)
        down_pair = ordered(down_keep, move_pair(down_give), 1)

        def halves(value):
            low, high = value[..., :hidden], value[..., hidden:]
            return jnp.where(first, low, high), jnp.where(first, high, low)

        def relative_rows(value):
            blocks = value.reshape(width, rows, value.shape[1])
            return jnp.concatenate(
                [
                    lax.dynamic_index_in_dim(blocks, (r - kr + nr) % nr * 2 + (c ^ kc), 0, False)
                    for kr in range(nr)
                    for kc in range(2)
                ]
            )

        gate_keep, gate_give = halves(relative_rows(gate_pre))
        up_keep, up_give = halves(relative_rows(up_pre))
        pre = [[jnp.stack((gate_keep, up_keep)), move_pair(jnp.stack((gate_give, up_give)))]]

        inputs = tokens_in.astype(F32)
        inv_rms = lax.rsqrt(jnp.mean(inputs * inputs, axis=1, keepdims=True) + 1e-05)
        normed = inputs * inv_rms
        terms, rest = [], inv_rms
        for _ in range(3):
            terms.append(lax.reduce_precision(rest, 8, 7))
            rest = rest - terms[-1]
        extra = jnp.concatenate(terms + [jnp.zeros((rows, 125), F32)], axis=1).astype(BF16)

        near = jnp.stack(
            [move_a(block_of(grad_out, k), k) if k else block_of(grad_out, 0) for k in range(na)]
        )
        every_out = []
        for kb in range(2):
            pieces = [near if kb == 0 and kr == 0 else move_br(near, kb, kr) for kr in range(nr)]
            mine = jnp.stack(pieces)
            both = jnp.stack((mine, move_core(mine)))
            every_out.append(both.transpose(2, 1, 0, 3, 4).reshape(na, group, pair))

        gate_w_keep, gate_w_give = halves(gate_weight)
        up_w_keep, up_w_give = halves(up_weight)
        weight_keep = jnp.stack((gate_w_keep, up_w_keep))
        weight_give = jnp.stack((gate_w_give, up_w_give))
        weight_give = move_pair(weight_give)
        weight_pair = jnp.zeros((2, pair, hidden), BF16)
        weight_pair = lax.dynamic_update_slice_in_dim(weight_pair, weight_keep, b * own, 1)
        weight_pair = lax.dynamic_update_slice_in_dim(weight_pair, weight_give, (1 - b) * own, 1)

        for _ in range(1, na):
            pre.append([move_a(pre[-1][kb], 1) for kb in range(2)])

        grads = [[None, None] for _ in range(na)]
        for kb in range(2):
            partial = lax.dot_general(
                every_out[kb].reshape(na * group, pair),
                down_pair,
                (((1,), (1,)), ((), ())),
                preferred_element_type=F32,
            ).astype(BF16).reshape(na, group, hidden)
            running = partial[1]
            for step in range(1, na):
                theirs = move_a(running, 1)
                running = (theirs.astype(F32) + partial[(step + 1) % na].astype(F32)).astype(BF16)
            grads[0][kb] = running
        late_inputs, late_extra, grads[0][1] = lax.optimization_barrier(
            (tokens_in, extra, grads[0][1])
        )
        near_normed = []
        for k in range(na):
            message = jnp.concatenate((block_of(late_inputs, k), late_extra), axis=1)
            if k:
                message = move_a(message, k)
            near_normed.append(message)
        for kb in range(2):
            for k in range(1, na):
                grads[k][kb] = move_a(grads[k - 1][kb], 1)

        pre_parts = [tuple(parts) for parts in pre]
        acts, norm_blocks = [], []
        gain_part = jnp.zeros((pair,), F32)
        for k in range(na):
            value = jnp.concatenate(pre_parts[k], axis=1).astype(F32)
            gate_value, up_value = value[0], value[1]
            gate_sigmoid = jax.nn.sigmoid(gate_value)
            gate_silu = gate_value * gate_sigmoid
            grad_act = jnp.concatenate(grads[k]).astype(F32)
            grad_gate = (
                grad_act * up_value * gate_sigmoid * (1.0 + gate_value * (1.0 - gate_sigmoid))
            ).astype(BF16)
            grad_up = (grad_act * gate_silu).astype(BF16)
            norm_part = jnp.einsum(
                "grf,gdf->rd",
                jnp.stack((grad_gate, grad_up)),
                weight_pair,
                preferred_element_type=F32,
            ).astype(BF16)
            norm_part = norm_part.reshape(2, nr, 2, rows, pair)
            across = move_core(norm_part[:, :, 1])
            cores = (norm_part[:, :, 0].astype(F32) + across.astype(F32)).astype(BF16)
            total = cores[0, 0].astype(F32)
            for kb in range(2):
                for kr in range(nr):
                    if kb or kr:
                        piece = cores[kb, kr]
                        piece = move_br(piece, kb, -kr)
                        total = total + piece.astype(F32)
            block = total.astype(BF16)
            norm_blocks.append(move_a(block, -k) if k else block)
            message, total = lax.optimization_barrier((near_normed[k], total))
            tail = message[:, pair:].astype(F32)
            their_inputs = message[:, :pair]
            their_inv = tail[:, 0:1] + tail[:, 1:2] + tail[:, 2:3]
            their_normed = their_inputs.astype(F32) * their_inv
            gain_part = gain_part + jnp.sum(total * their_normed, axis=0)

        for k in range(na):
            value = jnp.concatenate(pre_parts[k], axis=1).astype(F32)
            gate_value, up_value = value[0], value[1]
            acts.append((gate_value * jax.nn.sigmoid(gate_value) * up_value).astype(BF16))
        down_both = lax.dot_general(
            jnp.concatenate(acts),
            jnp.concatenate(every_out, axis=1).reshape(na * 2 * group, pair),
            (((0,), (0,)), ((), ())),
            preferred_element_type=F32,
        ).astype(BF16)
        low, high = down_both[:, :own], down_both[:, own:]
        give = jnp.where(first, high, low)
        cut = hidden * 3 // 4 // 16 * 16
        theirs = move_pair(give[:cut]), move_pair(give[cut:])
        down_grad = jnp.zeros((2 * hidden, own), BF16)
        mine = jnp.where(first, low, high)
        down_grad = lax.dynamic_update_slice_in_dim(down_grad, mine, b * hidden, 0)
        there = (1 - b) * hidden
        down_grad = lax.dynamic_update_slice_in_dim(down_grad, theirs[0], there, 0)
        down_grad = lax.dynamic_update_slice_in_dim(down_grad, theirs[1], there + cut, 0)

        gain = gain_part + move_core(gain_part)
        gain_sum = gain
        for kb in range(2):
            for kr in range(nr):
                if kb or kr:
                    gain_sum = gain_sum + move_br(gain, kb, kr)

        def natural(blocks, axis):
            twice = jnp.concatenate(blocks + blocks, axis=axis)
            return lax.dynamic_slice_in_dim(twice, (na - a) % na * pair, features, axis)

        gain_grad = natural([move_a(gain_sum, -k) if k else gain_sum for k in range(na)], 0)
        grad_norm = natural(norm_blocks, 1).astype(F32)
        scaled = grad_norm * norm_gain
        inner = jnp.mean(scaled * normed, axis=1, keepdims=True)
        step = inv_rms * (scaled - normed * inner)
        input_grad = (grad_out.astype(F32) + step).astype(BF16)
        return (input_grad, gain_grad, down_grad)

    return per_device


def solution(mesh):
    inner = make_per_device(mesh)

    return jax.shard_map(
        inner,
        mesh=mesh,
        in_specs=(
            P(("dp", "tensor"), None),
            P(("dp", "tensor"), None),
            P("dp", "tensor"),
            P("dp", "tensor"),
            P("dp", "tensor"),
            P("dp", "tensor"),
            P("tensor", "dp"),
            P(),
        ),
        out_specs=(P(("dp", "tensor"), None), P(), P("tensor", "dp")),
        check_vma=False,
    )
```
